32 devices in a mesh: groups: 2 (over y), dom: 4 (over z), shot: 4 (over x, core).
Axes of the slice: x: 2, y: 2, z: 4, core: 2. Of those that a mesh axis runs over, the one named last changes fastest.
Arguments:
- courant_sq: float32 [128, 128, 128], P(('groups', 'dom')), parts along dimension 0, may hold values from 0.05 to 0.19
- adjoint_init: float32 [8, 2, 64, 128, 128], P(('groups', 'shot'), None, 'dom'), parts along dimension 0, may hold values from -6 to 6
- forward_saved: bfloat16 [8, 6, 64, 128, 128], P(('groups', 'shot'), None, 'dom'), parts along dimension 0, may hold values from -4 to 4
- residual_traces: float32 [8, 4, 1024], P(('groups', 'shot')), parts along dimension 0, may hold values from -6 to 6
- receivers: int32 [8, 1024, 3], P(('groups', 'shot')), parts along dimension 0, may hold values from 0 to 127, as said below
- sources: int32 [8, 3], P(('groups', 'shot')), parts along dimension 0, may hold values from 0 to 127, as said below
Outputs:
- gradient: float32 [128, 128, 128], P(('groups', 'dom'), 'shot'), parts along dimension 0
- adjoint_final: float32 [8, 2, 64, 128, 128], P(('groups', 'shot'), None, 'dom'), parts along dimension 0
The draws below stay inside these ranges and needn't reach their ends.
There are 2 independent parts, one for each index of `groups`. The reference program is written for one: setup_inputs(seed, part) draws one part's arguments, and reference() takes and returns one part's arrays. A program takes and returns all parts, laid end to end along the dimension named above; each array names one. Nothing has to cross between parts.
Inputs may be any that keep to these rules, and one draw needn't show every extreme that they name: Each row holds the depth index (below 64), the first horizontal index (below 128) and the second (below 128) of a cell; receivers may share cells. `sources`: each row holds the depth index (below 64), the first horizontal index (below 128) and the second (below 128) of a cell.
All inputs are finite; a program needn't handle non-finite values.
Results may differ from the reference program's by a relative error of at most 0.0003.
Values sent between devices are 32-bit elements; how exact they have to be, the bound alone decides.
A program may use at most 64 MiB of HBM per device.

```python
import jax
import jax.numpy as jnp

NX = 128
NY = 128
REC = 1024
ITERS = 4
RADIUS = 6
NZ = 64
SHOTS = 4


def draw_courant_sq(key, part):
    shape = (NZ, NX, NY)
    values = jax.random.uniform(jax.random.fold_in(key, 31), shape, jnp.float32, 0.05, 0.19)
    return values


def draw_adjoint_init(key, part):
    shape = (SHOTS, 2, NZ, NX, NY)
    rough = jax.random.normal(jax.random.fold_in(key, 47), shape, jnp.float32)
    values = jnp.clip(rough, -6.0, 6.0)
    return values


def draw_receivers(key, part):
    limits = jnp.array([NZ, NX, NY], jnp.int32)
    return jax.random.randint(jax.random.fold_in(key, 11), (SHOTS, REC, 3), 0, limits).astype(jnp.int32)


def draw_sources(key, part):
    limits = jnp.array([NZ, NX, NY], jnp.int32)
    values = jax.random.randint(jax.random.fold_in(key, 23), (SHOTS, 3), 0, limits).astype(jnp.int32)
    if NZ >= max(NX, NY):
        values = values.at[0, 0].set(NZ - 1)
    elif NX >= NY:
        values = values.at[0, 1].set(NX - 1)
    else:
        values = values.at[0, 2].set(NY - 1)
    values = values.at[1, 1].set(0)
    return values.astype(jnp.int32)


def block_scale(own_key, extent, pieces, smallest, top_value):
    loudness = 1.0
    for position, blocks in pieces:
        draws = jax.random.uniform(jax.random.fold_in(jax.random.fold_in(own_key, 6), position), (blocks,), jnp.float32, smallest / len(pieces), top_value / len(pieces))
        loudness = loudness * jnp.repeat(jnp.exp(draws), extent[position] // blocks).reshape((-1,) + (1,) * (len(extent) - 1 - position))
    return loudness


def centred(stream_key, dims, scale, bound, shards=(), kind=jnp.bfloat16):
    values = jax.random.normal(stream_key, dims, jnp.float32) * scale
    if len(shards) > 0:
        values = block_scale(stream_key, dims, shards, -0.22, 0.18) * values
    return jnp.clip(values, min=-bound, max=bound).astype(kind)


def setup_inputs(seed: int = 0, part: int = 0) -> dict:
    streams_of = jax.random.split(jax.random.key(seed), 7)
    own_keys = jax.random.split(jax.random.fold_in(streams_of[6], part), 7)
    courant_sq = draw_courant_sq(jax.random.fold_in(jax.random.fold_in(streams_of[6], part), 71), part)
    adjoint_init = draw_adjoint_init(jax.random.fold_in(jax.random.fold_in(streams_of[6], part), 71), part)
    forward_saved = centred(own_keys[2], (SHOTS, ITERS + 2, NZ, NX, NY), 0.25, 4.0, ((0, 4), (2, 4)))
    residual_traces = centred(own_keys[3], (SHOTS, ITERS, REC), 1.0, 6.0, ((0, 4),), jnp.float32)
    receivers = draw_receivers(jax.random.fold_in(jax.random.fold_in(streams_of[6], part), 71), part)
    sources = draw_sources(jax.random.fold_in(jax.random.fold_in(streams_of[6], part), 71), part)
    return {"courant_sq": courant_sq, "adjoint_init": adjoint_init, "forward_saved": forward_saved, "residual_traces": residual_traces, "receivers": receivers, "sources": sources}


STENCIL_WEIGHTS = (-205.0 / 72.0, 8.0 / 5.0, -1.0 / 5.0, 8.0 / 315.0, -1.0 / 560.0)


def laplacian(field):
    size_z, size_x, size_y = field.shape
    padded = jnp.pad(field, 4)
    center = padded[4:4 + size_z, 4:4 + size_x, 4:4 + size_y]
    summed = 3.0 * STENCIL_WEIGHTS[0] * center
    for offset in range(1, 5):
        beside_all = padded[4 + offset:4 + offset + size_z, 4:4 + size_x, 4:4 + size_y]
        beside_all = beside_all + padded[4 - offset:4 - offset + size_z, 4:4 + size_x, 4:4 + size_y]
        beside_all = beside_all + padded[4:4 + size_z, 4 + offset:4 + offset + size_x, 4:4 + size_y]
        beside_all = beside_all + padded[4:4 + size_z, 4 - offset:4 - offset + size_x, 4:4 + size_y]
        beside_all = beside_all + padded[4:4 + size_z, 4:4 + size_x, 4 + offset:4 + offset + size_y]
        beside_all = beside_all + padded[4:4 + size_z, 4:4 + size_x, 4 - offset:4 - offset + size_y]
        summed = summed + STENCIL_WEIGHTS[offset] * beside_all
    return summed


def source_taper(source, depth_first, size_z, size_x, size_y):
    depth_gap = jnp.arange(size_z, dtype=jnp.int32) + depth_first - source[0]
    across_gap = jnp.arange(size_x, dtype=jnp.int32) - source[1]
    along_gap = jnp.arange(size_y, dtype=jnp.int32) - source[2]
    distance = (depth_gap * depth_gap)[:, None, None] + (across_gap * across_gap)[None, :, None] + (along_gap * along_gap)[None, None, :]
    return 1.0 - jnp.exp(-distance.astype(jnp.float32) / float(RADIUS * RADIUS))


def reference(courant_sq, adjoint_init, forward_saved, residual_traces, receivers, sources):
    size_z, size_x, size_y = courant_sq.shape
    gradient = jnp.zeros((size_z, size_x, size_y), jnp.float32)
    finals = []
    for shot_index in range(SHOTS):
        level_later = adjoint_init[shot_index, 0]
        level_now = adjoint_init[shot_index, 1]
        spots = receivers[shot_index]
        summed = jnp.zeros((size_z, size_x, size_y), jnp.float32)
        for section in range(ITERS - 1, -1, -1):
            level_next = 2.0 * level_now - level_later + courant_sq * laplacian(level_now)
            level_next = level_next.at[spots[:, 0], spots[:, 1], spots[:, 2]].add(residual_traces[shot_index, section])
            forward_accel = forward_saved[shot_index, section + 2].astype(jnp.float32) - 2.0 * forward_saved[shot_index, section + 1].astype(jnp.float32) + forward_saved[shot_index, section].astype(jnp.float32)
            summed = summed + level_next * forward_accel
            level_later, level_now = level_now, level_next
        gradient = gradient + source_taper(sources[shot_index], 0, size_z, size_x, size_y) * summed
        finals.append(jnp.stack([level_later, level_now]))
    return gradient, jnp.stack(finals)
```

```python
import functools

import jax
import jax.numpy as jnp
from jax import lax
from jax.experimental import pallas as pl
from jax.experimental.pallas import tpu as pltpu
from jax.sharding import PartitionSpec as P

ITERS = 4
RADIUS = 6
HALO = 4
PAD = 8

STENCIL_WEIGHTS = (-205.0 / 72.0, 8.0 / 5.0, -1.0 / 5.0, 8.0 / 315.0, -1.0 / 560.0)


def pieces_of(shot_n, rows):
    if shot_n == 4 and rows % 16 == 0:
        half = rows // 2
        return [(0, 0, half), (1, 0, half), (0, half, half), (1, half, half), (2, 0, rows), (3, 0, rows)]
    return [(i, 0, rows) for i in range(shot_n)]


def kernel(
    dom_n,
    shot_n,
    source_hbm,
    spot_hbm,
    trace_hbm,
    courant_hbm,
    init_hbm,
    fwd_hbm,
    grad_ref,
    final_ref,
    lev,
    courant,
    fwd,
    image,
    hot,
    columns,
    src,
    band,
    parts,
    source,
    spot,
    trace,
    in_sem,
    send_sem,
    recv_sem,
    part_recv,
):
    slab, size_x, size_y = courant.shape
    rows = size_x // shot_n
    n_rec = spot.shape[2]
    inner = slab - 2 * HALO
    pieces = pieces_of(shot_n, rows)
    me = lax.axis_index("dom")
    shot = lax.axis_index("shot")
    has_up = me > 0
    has_down = me < dom_n - 1
    paired = shot_n == 4

    def owner(i):
        i = i + 1
        if shot_n % 2:
            return lax.rem(shot + i, shot_n)
        pair = lax.rem(lax.div(shot, 2) + (i // 2 + i % 2) % (shot_n // 2), shot_n // 2)
        return pair * 2 + lax.rem(shot + i, 2)

    def target(i):
        return owner(2) if paired and i == 0 else owner(i)

    peers = (1, 2) if paired else range(shot_n - 1)
    barrier = pltpu.get_barrier_semaphore()

    @pl.when(has_up)
    def _():
        pl.semaphore_signal(barrier, inc=1, device_id={"dom": me - 1})

    @pl.when(has_down)
    def _():
        pl.semaphore_signal(barrier, inc=1, device_id={"dom": me + 1})

    for i in peers:
        pl.semaphore_signal(barrier, inc=1, device_id={"shot": owner(i)})

    across = pl.ds(PAD, size_x)

    def load_planes(first, count, sem):
        return pltpu.make_async_copy(
            init_hbm.at[1, pl.ds(first, count)],
            lev.at[1, pl.ds(HALO + first, count), across, :],
            in_sem.at[sem],
        )

    edge_loads = [load_planes(0, HALO, 0), load_planes(slab - HALO, HALO, 1)]
    spot_loads = [
        pltpu.make_async_copy(spot_hbm, spot, in_sem.at[2]),
        pltpu.make_async_copy(trace_hbm, trace, in_sem.at[3]),
    ]
    loads = [
        load_planes(HALO, inner, 4),
        pltpu.make_async_copy(init_hbm.at[0], lev.at[0, pl.ds(HALO, slab), across, :], in_sem.at[5]),
        pltpu.make_async_copy(courant_hbm, courant, in_sem.at[6]),
        pltpu.make_async_copy(fwd_hbm, fwd, in_sem.at[7]),
        pltpu.make_async_copy(source_hbm, source, in_sem.at[8]),
    ]
    for load in edge_loads + spot_loads + loads:
        load.start()

    gap = jnp.abs(
        lax.broadcasted_iota(jnp.int32, (size_y, size_y), 0)
        - lax.broadcasted_iota(jnp.int32, (size_y, size_y), 1)
    )
    weights = jnp.where(gap == 0, jnp.float32(3.0 * STENCIL_WEIGHTS[0]), jnp.float32(0.0))
    for offset in range(1, HALO + 1):
        weights = jnp.where(gap == offset, jnp.float32(STENCIL_WEIGHTS[offset]), weights)
    coarse = weights.astype(jnp.bfloat16)
    band[0:size_y, :] = coarse
    band[size_y : 2 * size_y, :] = coarse
    band[2 * size_y :, :] = (weights - coarse.astype(jnp.float32)).astype(jnp.bfloat16)

    for level in range(1, ITERS + 1):
        lev[level, HALO : HALO + slab, 0:PAD] = jnp.zeros((slab, PAD, size_y), jnp.float32)
        lev[level, HALO : HALO + slab, PAD + size_x :] = jnp.zeros(
            (slab, PAD, size_y), jnp.float32
        )

    def span(piece):
        strip, offset, count = pieces[piece]
        return pl.multiple_of(owner(strip) * rows + offset, 8), count

    def halo_copies(step, piece):
        level = step + 1
        first, count = span(piece)
        cut = pl.ds(pl.multiple_of(PAD + first, 8), count)
        upward = pltpu.make_async_remote_copy(
            src_ref=lev.at[level, pl.ds(HALO, HALO), cut, :],
            dst_ref=lev.at[level, pl.ds(HALO + slab, HALO), cut, :],
            send_sem=send_sem.at[0],
            recv_sem=recv_sem.at[step % 2, 0, piece],
            device_id={"dom": me - 1},
        )
        downward = pltpu.make_async_remote_copy(
            src_ref=lev.at[level, pl.ds(slab, HALO), cut, :],
            dst_ref=lev.at[level, pl.ds(0, HALO), cut, :],
            send_sem=send_sem.at[1],
            recv_sem=recv_sem.at[step % 2, 1, piece],
            device_id={"dom": me + 1},
        )
        return upward, downward

    def send_halo(step, piece):
        upward, downward = halo_copies(step, piece)

        @pl.when(has_up)
        def _():
            upward.start()

        @pl.when(has_down)
        def _():
            downward.start()

    def wait_halo(step, piece):
        upward, downward = halo_copies(step, piece)

        @pl.when(has_down)
        def _():
            upward.wait_recv()

        @pl.when(has_up)
        def _():
            downward.wait_recv()

    with jax.named_scope("edge_loads"):
        for load in edge_loads:
            load.wait()
    with jax.named_scope("barrier_wait"):
        pl.semaphore_wait(barrier, has_up.astype(jnp.int32) + has_down.astype(jnp.int32) + len(peers))
    for piece in range(len(pieces)):
        send_halo(0, piece)

    @pl.when(jnp.logical_not(has_up))
    def _():
        for level in range(1, ITERS + 1):
            lev[level, 0:HALO] = jnp.zeros((HALO, size_x + 2 * PAD, size_y), jnp.float32)

    @pl.when(jnp.logical_not(has_down))
    def _():
        for level in range(1, ITERS + 1):
            lev[level, HALO + slab :] = jnp.zeros((HALO, size_x + 2 * PAD, size_y), jnp.float32)

    for load in spot_loads:
        load.wait()

    with jax.named_scope("hot"):

        @pl.loop(0, slab)
        def _(z):
            row = lax.broadcasted_iota(jnp.int32, (size_x, n_rec), 0) + z * size_x
            same = row == (spot[0] - me * slab) * size_x + spot[1]
            hot[pl.ds(pl.multiple_of(z * size_x, size_x), size_x), :] = jnp.where(
                same, 1.0, 0.0
            ).astype(jnp.bfloat16)

        same = lax.broadcasted_iota(jnp.int32, (size_y, n_rec), 0) == spot[2]
        for section in range(ITERS):
            amount = trace[section : section + 1, :]
            high = amount.astype(jnp.bfloat16).astype(jnp.float32)
            columns[section, 0:size_y] = jnp.where(same, high, 0.0).astype(jnp.bfloat16)
            columns[section, size_y:] = jnp.where(same, amount - high, 0.0).astype(jnp.bfloat16)

    block = HALO * size_x
    blocks = slab // HALO

    def place(step, i):
        cut = pl.ds(pl.multiple_of(i * block, block), block)
        both = lax.dot_general(
            hot[cut, :],
            columns[ITERS - 1 - step],
            (((1,), (1,)), ((), ())),
            preferred_element_type=jnp.float32,
        )
        src[step, cut, :] = both[:, 0:size_y] + both[:, size_y:]

    def update(step, z, first, count, at):
        level = step + 1
        section = ITERS - 1 - step
        planes = HALO
        cut = pl.ds(pl.multiple_of(PAD + first, 8), count)
        plain = pl.ds(first, count)
        here = pl.ds(z, planes)
        store = pl.ds(at, planes)
        now = lev[level, pl.ds(HALO + z, planes), cut, :]
        flat = now.reshape(planes * count, size_y)
        high = flat.astype(jnp.bfloat16)
        low = (flat - high.astype(jnp.float32)).astype(jnp.bfloat16)
        total = lax.dot_general(
            jnp.concatenate([high, low, high], axis=1),
            band[...],
            (((1,), (0,)), ((), ())),
            preferred_element_type=jnp.float32,
        ).reshape(planes, count, size_y)
        for offset in range(1, HALO + 1):
            beside = (
                lev[level, pl.ds(HALO + z + offset, planes), cut, :]
                + lev[level, pl.ds(HALO + z - offset, planes), cut, :]
                + lev[level, pl.ds(HALO + z, planes), pl.ds(PAD + first + offset, count), :]
                + lev[level, pl.ds(HALO + z, planes), pl.ds(PAD + first - offset, count), :]
            )
            total = total + STENCIL_WEIGHTS[offset] * beside
        added = [
            src[step, pl.ds(pl.multiple_of((z + p) * size_x + first, 8), count), :]
            for p in range(planes)
        ]
        later = lev[level - 1, pl.ds(HALO + z, planes), cut, :]
        new = 2.0 * now - later + courant[here, plain, :] * total + jnp.stack(added)
        if step < ITERS - 1:
            lev[level + 1, pl.ds(HALO + z, planes), cut, :] = new
        if step >= ITERS - 2:
            final_ref[step - (ITERS - 2), here, plain, :] = new
        accel = (
            fwd[section + 2, here, plain, :].astype(jnp.float32)
            - 2.0 * fwd[section + 1, here, plain, :].astype(jnp.float32)
            + fwd[section, here, plain, :].astype(jnp.float32)
        )
        value = new * accel
        if step > 0:
            value = value + image[store, plain, :]
        if step == ITERS - 1:
            shape = (planes, count, size_y)
            dz = lax.broadcasted_iota(jnp.int32, shape, 0) + (me * slab + z - source[0])
            dx = lax.broadcasted_iota(jnp.int32, shape, 1) + (first - source[1])
            dy = lax.broadcasted_iota(jnp.int32, shape, 2) - source[2]
            distance = (dz * dz + dx * dx + dy * dy).astype(jnp.float32)
            value = value * (1.0 - jnp.exp(distance * (-1.0 / float(RADIUS * RADIUS))))
        image[store, plain, :] = value

    def interior(step, strips):
        @pl.loop(HALO, slab - HALO, step=HALO)
        def _(z):
            for strip in strips:
                first = pl.multiple_of(owner(strip) * rows, 8)
                update(step, z, first, rows, z + HALO)

    def edges(step, piece):
        first, count = span(piece)
        update(step, 0, first, count, 0)
        update(step, slab - HALO, first, count, HALO)

    def part_copy(slot, strip, at, planes, offset, count):
        return pltpu.make_async_remote_copy(
            src_ref=image.at[
                pl.ds(at, planes), pl.ds(pl.multiple_of(owner(strip) * rows + offset, 8), count), :
            ],
            dst_ref=parts.at[strip, pl.ds(at, planes), pl.ds(offset, count), :],
            send_sem=send_sem.at[2],
            recv_sem=part_recv.at[slot],
            device_id={"shot": target(strip)},
        )

    inner_parts = [part_copy(i, i, 2 * HALO, inner, 0, rows) for i in range(shot_n - 1)]
    edge_parts = {
        piece: part_copy(shot_n - 1 + piece, strip, 0, 2 * HALO, offset, count)
        for piece, (strip, offset, count) in enumerate(pieces)
        if strip < shot_n - 1
    }

    def relay(at, planes, offset, count, arrived, onward):
        arrived.wait_recv()
        here = pl.ds(at, planes)
        cut = pl.ds(pl.multiple_of(owner(1) * rows + offset, 8), count)
        image[here, cut, :] = image[here, cut, :] + parts[0, here, pl.ds(offset, count), :]
        onward.start()

    for i in range(blocks):
        with jax.named_scope("place0"):
            place(0, i)
    for load in loads:
        load.wait()

    half = shot_n // 2
    strips = list(range(shot_n))
    for step in range(ITERS - 1):
        jobs = [[] for _ in pieces]
        jobs[0].append(functools.partial(interior, step, strips[:half]))
        jobs[1 % len(pieces)].append(functools.partial(interior, step, strips[half:]))
        for i in range(blocks):
            jobs[min(2 + i, max(len(pieces) - 2, 0))].append(functools.partial(place, step + 1, i))
        for piece in range(len(pieces)):
            with jax.named_scope(f"wait{step}_{piece}"):
                wait_halo(step, piece)
            edges(step, piece)
            send_halo(step + 1, piece)
            with jax.named_scope(f"jobs{step}_{piece}"):
                for job in jobs[piece]:
                    job()

    step = ITERS - 1
    with jax.named_scope("interior3"):
        if paired:
            interior(step, [0])
            inner_parts[0].start()
            interior(step, [1, 2])
            inner_parts[2].start()
            interior(step, [3])
            relay(2 * HALO, inner, 0, rows, inner_parts[0], inner_parts[1])
        else:
            for i in range(shot_n):
                interior(step, [i])
                if i < shot_n - 1:
                    inner_parts[i].start()

    pending = []
    for piece, (strip, offset, count) in enumerate(pieces):
        with jax.named_scope(f"wait{step}_{piece}"):
            wait_halo(step, piece)
        edges(step, piece)
        if strip < shot_n - 1 and not (paired and strip == 1):
            edge_parts[piece].start()
        if paired and strip == 1:
            pending.append(piece)
        if paired and (strip == 0 or piece == max(p for p in edge_parts if pieces[p][0] == 1)):
            while pending:
                onward = pending.pop(0)
                _, offset, count = pieces[onward]
                with jax.named_scope(f"relay{onward}"):
                    relay(0, 2 * HALO, offset, count, edge_parts[pieces.index((0, offset, count))], edge_parts[onward])

    mine = pl.multiple_of(shot * rows, 8)
    adding = (2, 1) if paired else range(shot_n - 1)

    def finish(at, planes, z, offset, count):
        value = image[pl.ds(at, planes), pl.ds(pl.multiple_of(mine + offset, 8), count), :]
        for i in adding:
            value = value + parts[i, pl.ds(at, planes), pl.ds(offset, count), :]
        grad_ref[pl.ds(z, planes), pl.ds(offset, count), :] = value

    with jax.named_scope("final_inner"):
        for i in adding:
            inner_parts[i].wait_recv()
        finish(2 * HALO, inner, HALO, 0, rows)
    with jax.named_scope("final_edge"):
        for i in adding:
            for piece in edge_parts:
                if pieces[piece][0] == i:
                    edge_parts[piece].wait_recv()
        finish(0, HALO, 0, 0, rows)
        finish(HALO, HALO, slab - HALO, 0, rows)

    whole = lev.at[0, pl.ds(0, ITERS * HALO), across, :]
    sent = [
        pltpu.make_async_remote_copy(
            src_ref=whole,
            dst_ref=whole,
            send_sem=send_sem.at[i],
            recv_sem=recv_sem.at[0, i, 0],
            device_id={"dom": me + 2 * i - 1},
        )
        for i in range(2)
    ]

    @pl.when(has_up)
    def _():
        sent[0].wait_send()

    @pl.when(has_down)
    def _():
        sent[1].wait_send()

    pltpu.make_async_remote_copy(
        src_ref=parts,
        dst_ref=parts,
        send_sem=send_sem.at[2],
        recv_sem=part_recv.at[0],
        device_id={"shot": owner(0)},
    ).wait_send()


def flush(grad_ref, final_ref, grad_out, final_out, sem):
    copies = [pltpu.make_async_copy(grad_ref, grad_out, sem.at[0])]
    for i in range(final_ref.shape[0]):
        copies.append(pltpu.make_async_copy(final_ref.at[i], final_out.at[i], sem.at[1 + i]))
    for copy in copies:
        copy.start()
    for copy in copies:
        copy.wait()


def per_device(
    dom_n, shot_n, courant_sq, adjoint_init, forward_saved, residual_traces, receivers, sources
):
    slab, size_x, size_y = courant_sq.shape
    n_rec = receivers.shape[1]
    rows = size_x // shot_n
    pieces = pieces_of(shot_n, rows)
    spot = jnp.transpose(receivers, (2, 0, 1))
    hbm = pl.BlockSpec(memory_space=pl.ANY)
    vmem = pl.BlockSpec(memory_space=pltpu.VMEM)
    gradient, final = pl.pallas_call(
        functools.partial(kernel, dom_n, shot_n),
        out_shape=(
            pltpu.VMEM((slab, rows, size_y), jnp.float32),
            pltpu.VMEM((2, slab, size_x, size_y), jnp.float32),
        ),
        in_specs=[hbm] * 6,
        out_specs=(vmem, vmem),
        scratch_shapes=[
            pltpu.VMEM((ITERS + 1, slab + 2 * HALO, size_x + 2 * PAD, size_y), jnp.float32),
            pltpu.VMEM((slab, size_x, size_y), jnp.float32),
            pltpu.VMEM((ITERS + 2, slab, size_x, size_y), jnp.bfloat16),
            pltpu.VMEM((slab, size_x, size_y), jnp.float32),
            pltpu.VMEM((slab * size_x, n_rec), jnp.bfloat16),
            pltpu.VMEM((ITERS, 2 * size_y, n_rec), jnp.bfloat16),
            pltpu.VMEM((ITERS, slab * size_x, size_y), jnp.float32),
            pltpu.VMEM((3 * size_y, size_y), jnp.bfloat16),
            pltpu.VMEM((shot_n - 1, slab, rows, size_y), jnp.float32),
            pltpu.SMEM(sources.shape[1:], jnp.int32),
            pltpu.VMEM(spot.shape, jnp.int32),
            pltpu.VMEM(residual_traces.shape[1:], jnp.float32),
            pltpu.SemaphoreType.DMA((9,)),
            pltpu.SemaphoreType.DMA((3,)),
            pltpu.SemaphoreType.DMA((2, 2, len(pieces))),
            pltpu.SemaphoreType.DMA((shot_n - 1 + len(pieces),)),
        ],
        compiler_params=pltpu.CompilerParams(
            collective_id=0, has_side_effects=True, vmem_limit_bytes=56 * 1024 * 1024
        ),
    )(
        sources[0],
        spot,
        residual_traces[0],
        courant_sq,
        adjoint_init[0],
        forward_saved[0],
    )
    gradient, final = pl.pallas_call(
        flush,
        out_shape=(
            jax.ShapeDtypeStruct(gradient.shape, jnp.float32),
            jax.ShapeDtypeStruct(final.shape, jnp.float32),
        ),
        in_specs=[vmem, vmem],
        out_specs=(hbm, hbm),
        scratch_shapes=[pltpu.SemaphoreType.DMA((3,))],
        compiler_params=pltpu.CompilerParams(vmem_limit_bytes=1024 * 1024),
    )(gradient, final)
    return gradient, final[None]


def solution(mesh):
    placed = (
        P(("groups", "dom"), None, None),
        P(("groups", "shot"), None, "dom", None, None),
        P(("groups", "shot"), None, "dom", None, None),
        P(("groups", "shot"), None, None),
        P(("groups", "shot"), None, None),
        P(("groups", "shot"), None),
    )
    return jax.shard_map(
        functools.partial(per_device, mesh.shape["dom"], mesh.shape["shot"]),
        mesh=mesh,
        in_specs=placed,
        out_specs=(
            P(("groups", "dom"), "shot", None),
            P(("groups", "shot"), None, "dom", None, None),
        ),
        check_vma=False,
    )
```
